32 devices in a mesh: gx: 8 (over z, y), gy: 4 (over x, core).
Axes of the slice: x: 2, y: 2, z: 4, core: 2. Of those that a mesh axis runs over, the one named last changes fastest.
Arguments:
- coarse_send: bfloat16 [8, 35, 4096], P('gx', None, 'gy'), may hold values from -6 to 6
- coarse_flux: float32 [8, 35, 1024], P('gx', None, 'gy'), may hold values from -6 to 6
- patch_owner: int32 [8], replicated, may hold values from 0 to 15, as said below
- velocity: float32 [3], replicated, may hold values from -0.6 to 0.6
- diffusivity: float32 [35], replicated, may hold values from 0.03 to 0.15
- stoich: float32 [35, 35], replicated, may hold values from -1 to 1
Outputs:
- fine_state: float32 [16, 35, 32768], P('gx', None, 'gy')
- reflux: float32 [8, 35, 1024], P('gx', None, 'gy')
The draws below stay inside these ranges and needn't reach their ends.
Inputs may be any that keep to these rules, and one draw needn't show every extreme that they name: `patch_owner`: the 8 entries are distinct; slot s belongs to owner group s // 2, the group of index s // 2 along gx; a group owns 0, 1 or 2 patches, and at least one group owns exactly 2.
All inputs are finite; a program needn't handle non-finite values.
Results may differ from the reference program's by a relative error of at most 0.0003.
Values may be sent and summed in bfloat16 or wider, within the bound.
A program may use at most 128 MiB of HBM per device.

```python
import math
import jax
import jax.numpy as jnp
from jax import lax

FIELDS = 35
CB = 16
SEND = 1
OWN = 2
NP = 8
NO = 16


def draw_patch_owner(key, part):
    key_perm, key_bits = jax.random.split(jax.random.fold_in(key, 17), 2)
    groups_total = NP // SEND
    half_way = groups_total // 2
    partner = jax.random.permutation(key_perm, groups_total).astype(jnp.int32)
    first_value = partner[0]
    partner = jnp.where(partner == half_way, first_value, partner).astype(jnp.int32)
    partner = partner.at[0].set(half_way).astype(jnp.int32)
    moved = jax.random.randint(key_bits, (NP,), 0, 2).astype(jnp.int32)
    patch_index = jnp.arange(NP, dtype=jnp.int32)
    source_group = (patch_index // SEND).astype(jnp.int32)
    within = (patch_index % SEND).astype(jnp.int32)
    moved = jnp.where(source_group == 0, 1, jnp.where(source_group == half_way, 0, moved)).astype(jnp.int32)
    target = jnp.where(moved == 1, partner[source_group], source_group).astype(jnp.int32)
    return (target * OWN + moved * SEND + within).astype(jnp.int32)


def block_scale(rng, dims, cuts, smallest, top_value):
    gain = 1.0
    for dim, shards_of in cuts:
        heights = jax.random.uniform(jax.random.fold_in(jax.random.fold_in(rng, 6), dim), (shards_of,), jnp.float32, smallest / len(cuts), top_value / len(cuts))
        gain = gain * jnp.repeat(jnp.exp(heights), dims[dim] // shards_of).reshape((-1,) + (1,) * (len(dims) - 1 - dim))
    return gain


def bell_draw(rng, shape, width, bound, shards=(), kind=jnp.bfloat16):
    gain = block_scale(rng, shape, shards, -0.22, 0.18) if shards else 1.0
    drawn = jax.random.normal(rng, shape, jnp.float32) * width * gain
    return jnp.minimum(jnp.maximum(drawn, -bound), bound).astype(kind)


def setup_inputs(seed: int = 0) -> dict:
    splits = jax.random.split(jax.random.key(seed), 7)
    coarse_send = bell_draw(splits[0], (NP, FIELDS, CB * CB * CB), 1.0, 6.0, ((0, 8), (2, 4)))
    coarse_flux = bell_draw(splits[1], (NP, FIELDS, CB * 4 * CB), 1.0, 6.0, ((0, 8), (2, 4)), jnp.float32)
    patch_owner = draw_patch_owner(jax.random.fold_in(splits[6], 71), 0)
    velocity = jnp.clip(jax.random.uniform(splits[3], (3,), jnp.float32, -0.6, 0.6), -0.6, 0.6)
    diffusivity = jnp.clip(jnp.exp(jax.random.uniform(splits[4], (FIELDS,), jnp.float32, math.log(0.03), math.log(0.15))), 0.03, 0.15)
    stoich = bell_draw(splits[5], (FIELDS, FIELDS), FIELDS ** -0.5, 1.0, (), jnp.float32)
    return dict(coarse_send=coarse_send, coarse_flux=coarse_flux, patch_owner=patch_owner, velocity=velocity, diffusivity=diffusivity, stoich=stoich)


time_step = 0.25
heat_gain = 2.0
highest = lax.Precision.HIGHEST


def axis_slope(values, axis):
    moved = jnp.moveaxis(values, axis, 0)
    middle = (moved[2:] - moved[:-2]) * 0.5
    joined = jnp.concatenate([moved[1:2] - moved[0:1], middle, moved[-1:] - moved[-2:-1]], 0)
    return jnp.moveaxis(joined, 0, axis)


def spread(values):
    return values[..., :, None, :, None, :, None]


def refine(coarse, slope_z, slope_y, slope_x):
    offsets = jnp.array([-0.5, 0.5], jnp.float32)
    leading = coarse.shape[:-3]
    depth, height, breadth = coarse.shape[-3:]
    shift_y = offsets[:, None, None]
    shift_z = offsets[:, None, None, None, None]
    terms = spread(slope_x) * offsets + spread(slope_y) * shift_y + spread(slope_z) * shift_z
    fine_cells = spread(coarse) + terms * 0.5
    return fine_cells.reshape(leading + (2 * depth, 2 * height, 2 * breadth))


def face_flux(left_side, right_side, speed, diffuse):
    return speed * (left_side + right_side) * 0.5 - diffuse * (right_side - left_side)


def tendency(padded_layers, cells, velocity, diffusivity, stoich):
    diffuse = diffusivity[:, None, None, None]
    padded_cols = jnp.concatenate([cells[..., :1], cells, cells[..., -1:]], -1)
    padded_rows = jnp.concatenate([cells[..., :1, :], cells, cells[..., -1:, :]], -2)
    flux_cols = face_flux(padded_cols[..., :-1], padded_cols[..., 1:], velocity[0], diffuse)
    flux_rows = face_flux(padded_rows[..., :-1, :], padded_rows[..., 1:, :], velocity[1], diffuse)
    flux_layers = face_flux(padded_layers[..., :-1, :, :], padded_layers[..., 1:, :, :], velocity[2], diffuse)
    outflow = (flux_cols[..., 1:] - flux_cols[..., :-1]) + (flux_rows[..., 1:, :] - flux_rows[..., :-1, :]) + (flux_layers[..., 1:, :, :] - flux_layers[..., :-1, :, :])
    reaction_rate = cells * jax.nn.sigmoid(heat_gain * cells[..., 0:1, :, :, :])
    source = jnp.einsum('fg,...gzyx->...fzyx', stoich, reaction_rate, precision=highest)
    side_fluxes = (flux_cols[..., 0], flux_cols[..., -1], flux_rows[..., 0, :], flux_rows[..., -1, :])
    return source - outflow, side_fluxes


def average_sides(earlier, later_sides):
    return jnp.stack([(earlier[0] + later_sides[0]) * 0.5, (earlier[1] + later_sides[1]) * 0.5, (earlier[2] + later_sides[2]) * 0.5, (earlier[3] + later_sides[3]) * 0.5], -2)


def coarsen_faces(register):
    leading = register.shape[:-3]
    depth = register.shape[-3] // 2
    along = register.shape[-1] // 2
    split_faces = register.reshape(leading + (depth, 2, 4, along, 2))
    return (split_faces[..., 0, :, :, 0] + split_faces[..., 0, :, :, 1] + split_faces[..., 1, :, :, 0] + split_faces[..., 1, :, :, 1]) * 0.25


def extend_edge(cells):
    return jnp.concatenate([cells[..., :1, :, :], cells, cells[..., -1:, :, :]], -3)


def reference(coarse_send, coarse_flux, patch_owner, velocity, diffusivity, stoich):
    def one_patch(inputs):
        coarse_block, face_values = inputs
        coarse = coarse_block.astype(jnp.float32).reshape(FIELDS, CB, CB, CB)
        fine_cells = refine(coarse, axis_slope(coarse, 1), axis_slope(coarse, 2), axis_slope(coarse, 3))
        change, first_sides = tendency(extend_edge(fine_cells), fine_cells, velocity, diffusivity, stoich)
        section_state = fine_cells + time_step * change
        second, second_sides = tendency(extend_edge(section_state), section_state, velocity, diffusivity, stoich)
        final_state = fine_cells + (time_step * 0.5) * (change + second)
        register = average_sides(first_sides, second_sides)
        corrected = coarsen_faces(register) - face_values.reshape(FIELDS, CB, 4, CB)
        return final_state.reshape(FIELDS, -1), corrected.reshape(FIELDS, -1)

    fine_all, reflux = lax.map(one_patch, (coarse_send, coarse_flux))
    fine_state = jnp.zeros((NO,) + fine_all.shape[1:], jnp.float32).at[patch_owner].set(fine_all)
    return fine_state, reflux
```

```python
import functools

import jax
import jax.numpy as jnp
import numpy as np
from jax import lax
from jax.experimental import pallas as pl
from jax.experimental.pallas import tpu as pltpu
from jax.sharding import PartitionSpec as P

time_step = 0.25
LANES = 128


def round_up(count, step):
    return -(-count // step) * step


def refine_matrix(edge):
    fine = 2 * edge
    copy_1d = np.zeros((edge, fine), np.float32)
    slope_1d = np.zeros((edge, fine), np.float32)
    for j in range(fine):
        i, sign = j // 2, (j % 2 - 0.5) * 0.5
        copy_1d[i, j] = 1.0
        low, high = max(i - 1, 0), min(i + 1, edge - 1)
        scale = sign * (0.5 if high - low == 2 else 1.0)
        slope_1d[high, j] += scale
        slope_1d[low, j] -= scale
    copies = np.einsum("ab,cd->acbd", copy_1d, copy_1d)
    shape = (edge * edge, fine * fine)
    planar = copies + np.einsum("ab,cd->acbd", copy_1d, slope_1d) + np.einsum("ab,cd->acbd", slope_1d, copy_1d)
    return np.concatenate([planar.reshape(shape), copies.reshape(shape)], 1)


def side_matrix(edge):
    fine = 2 * edge
    pick = np.zeros((fine, fine, 4, edge), np.float32)
    for along in range(fine):
        pick[along, 0, 0, along // 2] = 1.0
        pick[along, fine - 1, 1, along // 2] = 1.0
        pick[0, along, 2, along // 2] = 1.0
        pick[fine - 1, along, 3, along // 2] = 1.0
    pick = pick.reshape(fine * fine, 4 * edge)
    return np.tile(pick, (1, max(1, LANES // (4 * edge))))


def split_halves(values):
    high = values.astype(jnp.bfloat16)
    low = (values - high.astype(jnp.float32)).astype(jnp.bfloat16)
    return high, low


def react_layer(source, index, react):
    rows, width = source.shape[1:]
    field_rows = react.shape[1] // 3
    rate = 1.0 / (1.0 + jnp.exp(-2.0 * source[index, 0:1, :]))
    reacting = source[index] * rate
    reacting = jnp.concatenate([reacting, jnp.zeros((field_rows - rows, width), jnp.float32)], 0)
    high, low = split_halves(reacting)
    return jnp.dot(react[...], jnp.concatenate([high, high, low], 0), preferred_element_type=jnp.float32)


def unrolled_layers(source, start, count, coefs, react, fine, use):
    for layer in range(count):
        produced = react_layer(source, start + layer, react)
        use(layer, step_layer(source, start + layer, coefs, produced, fine))


def run_layers(source, start, count, coefs, react, produced, fine, use):
    produced[...] = react_layer(source, start, react)

    @pl.loop(0, count)
    def _(layer):
        following = react_layer(source, start + layer + 1, react)
        use(layer, step_layer(source, start + layer, coefs, produced, fine))
        produced[...] = following


def step_layer(source, index, coefs, produced, fine):
    rows, width = source.shape[1:]
    tiles = width // LANES
    lane = lax.broadcasted_iota(jnp.int32, (8, LANES), 1)
    column = lax.rem(lane, fine)
    first_x, last_x = column == 0, column == fine - 1
    up_mask, down_mask = lane < LANES - fine, lane >= fine
    pieces = []
    for group in range(rows // 8):
        band = slice(8 * group, 8 * group + 8)
        cells = [source[index, band, LANES * t : LANES * (t + 1)] for t in range(tiles)]
        raised = [pltpu.roll(c, LANES - fine, 1) for c in cells]
        lowered = [pltpu.roll(c, fine, 1) for c in cells]
        across = []
        for t in range(tiles):
            span = slice(LANES * t, LANES * (t + 1))
            c = cells[t]
            x_high = jnp.where(last_x, c, pltpu.roll(c, LANES - 1, 1))
            x_low = jnp.where(first_x, c, pltpu.roll(c, 1, 1))
            y_high = jnp.where(up_mask, raised[t], raised[t + 1] if t + 1 < tiles else c)
            y_low = jnp.where(down_mask, lowered[t], lowered[t - 1] if t else c)
            z_high = source[index + 1, band, span]
            z_low = source[index - 1, band, span]
            total = coefs[0, band, :] * x_high + coefs[1, band, :] * x_low
            total += coefs[2, band, :] * y_high + coefs[3, band, :] * y_low
            total += coefs[4, band, :] * z_high + coefs[5, band, :] * z_low
            total += coefs[6, band, :] * c
            across.append(total + produced[band, span])
        pieces.append(across)
    return pieces


def store_layer(target, index, pieces):
    for group, across in enumerate(pieces):
        for t, value in enumerate(across):
            target[index, 8 * group : 8 * group + 8, LANES * t : LANES * (t + 1)] = value


def fill_layers(coarse, matrix, spread, state, at_bottom, at_top):
    held, padded_rows, cells = coarse.shape
    rows, width = state.shape[1:]
    flat = coarse[...].reshape(held * padded_rows, cells)
    spread[...] = jnp.dot(flat, matrix[...], preferred_element_type=jnp.float32)

    def copies(layer):
        return spread[pl.ds(layer * padded_rows, rows), width:]

    @pl.when(at_bottom)
    def _():
        spread[pl.ds(1 * padded_rows, rows), width:] = 2.0 * copies(2) - copies(3)

    @pl.when(at_top)
    def _():
        top = held - 2
        spread[pl.ds(top * padded_rows, rows), width:] = 2.0 * copies(top - 1) - copies(top - 2)

    for layer in range(1, held - 1):
        planar = spread[pl.ds(layer * padded_rows, rows), :width]
        slope = (copies(layer + 1) - copies(layer - 1)) * 0.125
        state[2 * layer - 2] = planar - slope
        state[2 * layer - 1] = planar + slope

    @pl.when(at_bottom)
    def _():
        state[1] = state[2]

    @pl.when(at_top)
    def _():
        state[2 * held - 6] = state[2 * held - 7]


def pencil_ends():
    pencil = lax.axis_index("gy")
    return pencil == 0, pencil == lax.axis_size("gy") - 1


def prepare(velocity, diffusivity, stoich, coefs, react, table):
    fields = stoich.shape[0]
    rows = coefs.shape[1]
    part = react.shape[1] // 3
    table[...] = jnp.zeros(table.shape, jnp.float32)
    table[:fields, :fields] = stoich[...] * time_step
    scaled = table[...]
    high = scaled.astype(jnp.bfloat16).astype(jnp.float32)
    low = scaled - high
    joined = high + pltpu.roll(low, part, 1) + pltpu.roll(high, 2 * part, 1)
    react[...] = joined[:, : 3 * part].astype(jnp.bfloat16)
    table[...] = jnp.zeros(table.shape, jnp.float32)
    table[0:1, :fields] = diffusivity[...]
    shape = (rows, LANES)
    diagonal = lax.broadcasted_iota(jnp.int32, shape, 0) == lax.broadcasted_iota(jnp.int32, shape, 1)
    line = jnp.broadcast_to(table[0:1, :LANES], shape)
    column = jnp.sum(jnp.where(diagonal, line, 0.0), 1, keepdims=True)
    diffuse = jnp.broadcast_to(column, shape)
    for dim in range(3):
        half_speed = velocity[dim] * 0.5
        coefs[2 * dim] = (diffuse - half_speed) * time_step
        coefs[2 * dim + 1] = (diffuse + half_speed) * time_step
    coefs[6] = 1.0 - 6.0 * time_step * diffuse


def prepared(fields):
    rows, padded_rows = round_up(fields, 8), round_up(fields, 16)
    return (
        jax.ShapeDtypeStruct((7, rows, LANES), jnp.float32),
        jax.ShapeDtypeStruct((rows, 3 * padded_rows), jnp.bfloat16),
    ), [pltpu.VMEM((rows, round_up(3 * padded_rows, LANES)), jnp.float32)]


def fine_kernel(
    fine, coarse, matrix, coefs, react, reflux, out, reflux_out, spread, state, middle, ready, sems, reflux_sem,
):
    reflux_copy = pltpu.make_async_copy(reflux, reflux_out, reflux_sem.at[0])
    reflux_copy.start()
    at_bottom, at_top = pencil_ends()
    slots = out.shape[2] * LANES // state.shape[2]
    fields = out.shape[0]
    layers = out.shape[1]
    step = out.shape[2]

    def copy_out(layer):
        return pltpu.make_async_copy(
            ready.at[layer],
            out.at[:, layer],
            sems.at[layer],
        )

    for slot in range(slots):
        fill_layers(coarse.at[slot], matrix, spread, state, at_bottom, at_top)
        def to_middle(layer, pieces):
            store_layer(middle, layer, pieces)

        unrolled_layers(state, 1, layers + 2, coefs, react, fine, to_middle)

        @pl.when(at_bottom)
        def _():
            middle[0] = middle[1]

        @pl.when(at_top)
        def _():
            middle[layers + 1] = middle[layers]

        def to_output(layer, pieces):
            for group, across in enumerate(pieces):
                low, high = 8 * group, min(8 * group + 8, fields)
                for t, value in enumerate(across):
                    span = slice(LANES * t, LANES * (t + 1))
                    half = (value + state[layer + 2, low : low + 8, span]) * 0.5
                    lines = ready.at[layer].reshape(fields * step, LANES)
                    lines[pl.ds(low * step + t * slots + slot, high - low, stride=step), :] = half[: high - low]

            if slot == slots - 1:
                copy_out(layer).start()

        unrolled_layers(middle, 1, layers, coefs, react, fine, to_output)

    for layer in range(layers):
        copy_out(layer).wait()
    reflux_copy.wait()


def side_sums(fine, coarse, matrix, coefs, react, sides, velocity, flux, out, produced, spread, state, sums):
    at_bottom, at_top = pencil_ends()
    fields = out.shape[0]
    rows, width = state.shape[1:]
    layers = state.shape[0] - 4
    fill_layers(coarse, matrix, spread, state, at_bottom, at_top)

    def to_sums(layer, pieces):
        for group, across in enumerate(pieces):
            band = slice(8 * group, 8 * group + 8)
            for t, value in enumerate(across):
                span = slice(LANES * t, LANES * (t + 1))
                sums[layer, band, span] = value + state[layer + 2, band, span]

    run_layers(state, 2, layers, coefs, react, produced, fine, to_sums)
    pads = jnp.zeros((round_up(rows, 16) - rows, width), jnp.float32)
    halves = []
    for pair in range(layers // 2):
        high, low = split_halves(jnp.concatenate([sums[2 * pair] + sums[2 * pair + 1], pads], 0))
        halves += [high, low]
    picked = jnp.dot(jnp.concatenate(halves, 0), sides[...], preferred_element_type=jnp.float32)
    step = rows + pads.shape[0]
    each = [
        picked[2 * step * i : 2 * step * i + rows] + picked[2 * step * i + step : 2 * step * i + step + rows]
        for i in range(layers // 2)
    ]
    span = sides.shape[1]
    per_tile = span // (fine * 2)
    lane = lax.broadcasted_iota(jnp.int32, (rows, span), 1)
    for tile in range(len(each) // per_tile):
        value = each[tile * per_tile]
        for i in range(1, per_tile):
            value = jnp.where(lane >= i * fine * 2, each[tile * per_tile + i], value)
        along_x = lax.rem(lane, fine * 2) < fine
        value = value * jnp.where(along_x, velocity[0] * 0.125, velocity[1] * 0.125)
        out[:, tile, :] = value[:fields] - flux[:, tile, :]


def route_kernel(
    fine, owner_hbm, velocity_hbm, own_hbm, diffusivity_hbm, stoich_hbm, flux_hbm, matrix_hbm, sides_hbm,
    held, reflux, coefs, react, matrix, table, produced, spread, state, sums, mine,
    owner, velocity, own, diffusivity, stoich, flux, sides, w_sems,
    padded, outgoing, edges, arrived, chosen, landed, a_send, a_recv, h_send, h_recv, b_send, b_recv,
):
    me, pencil = lax.axis_index("gx"), lax.axis_index("gy")
    groups, pencils = lax.axis_size("gx"), lax.axis_size("gy")
    fields = own.shape[0]
    rows = padded.shape[0]
    half = groups // 2
    pairs = (
        (own_hbm, own), (owner_hbm, owner), (velocity_hbm, velocity), (diffusivity_hbm, diffusivity),
        (stoich_hbm, stoich), (flux_hbm, flux), (matrix_hbm, matrix), (sides_hbm, sides),
    )
    fetches = [pltpu.make_async_copy(source, target, w_sems.at[i]) for i, (source, target) in enumerate(pairs)]
    for copy in fetches:
        copy.start()
    own_in, owner_in, small_in, weights = fetches[0], fetches[1], fetches[2:5], fetches[5:]
    slots = chosen.shape[1]
    has_low, has_high = pencil > 0, pencil < pencils - 1
    around = [lax.rem(me + k, groups) for k in range(groups)]

    barrier = pltpu.get_barrier_semaphore()

    def greet(group, to):
        pl.semaphore_signal(barrier, inc=1, device_id=(group, to), device_id_type=pl.DeviceIdType.MESH)

    for group in around[1:]:
        greet(group, pencil)

    @pl.when(has_low)
    def _():
        greet(me, pencil - 1)

    @pl.when(has_high)
    def _():
        greet(me, pencil + 1)

    own_in.wait()
    padded[rows - 16 :, :] = jnp.zeros((16, padded.shape[1]), jnp.float32)
    padded[:fields, :] = own[...].astype(jnp.float32)
    for piece in range(groups):
        outgoing[piece] = padded[:, LANES * piece : LANES * (piece + 1)].astype(jnp.bfloat16)
    arrived[me] = outgoing[me]
    arrived[groups] = jnp.zeros(arrived.shape[1:], jnp.bfloat16)

    owner_in.wait()
    sources = []
    for group in around:
        for o in range(slots):
            slot = group * slots + o
            source = jnp.int32(groups)
            for q in range(groups):
                source = jnp.where(owner[q] == slot, q, source)
            sources.append(source)

    for copy in small_in:
        copy.wait()
    prepare(velocity, diffusivity, stoich, coefs, react, table)
    near = groups - 1
    pl.semaphore_wait(barrier, near + (has_low.astype(jnp.int32) + has_high.astype(jnp.int32)))

    def send(src, dst, out_sem, in_sem, group, to):
        return pltpu.make_async_remote_copy(
            src_ref=src, dst_ref=dst, send_sem=out_sem, recv_sem=in_sem,
            device_id=(group, to), device_id_type=pl.DeviceIdType.MESH,
        )

    first = [
        send(outgoing.at[group], arrived.at[me], a_send.at[k], a_recv.at[me], group, pencil)
        for k, group in enumerate(around)
    ]
    to_high = send(outgoing.at[half:], edges.at[:half], h_send.at[0], h_recv.at[0], me, pencil + 1)
    to_low = send(outgoing.at[:half], edges.at[half:], h_send.at[1], h_recv.at[1], me, pencil - 1)
    for copy in first[1:]:
        copy.start()
    pl.when(has_high)(to_high.start)
    pl.when(has_low)(to_low.start)
    for group in around[1:]:
        send(outgoing.at[group], arrived.at[group], a_send.at[0], a_recv.at[group], group, pencil).wait_recv()

    for k, group in enumerate(around):
        for o in range(slots):
            chosen[group, o] = arrived[sources[k * slots + o]]
    landed[half + me] = chosen[me]

    second = [
        send(chosen.at[group], landed.at[half + me], b_send.at[0, k], b_recv.at[half + me], group, pencil)
        for k, group in enumerate(around)
    ]
    for copy in second[1:]:
        copy.start()

    relays = []
    for k, group in enumerate(around):
        piece = landed.at[half + group]
        goes_low = jnp.logical_and(has_low, group < half)
        goes_high = jnp.logical_and(has_high, group >= half)
        over, under = half + groups + group, lax.rem(group + half, groups)
        relays.append((goes_low, send(piece, landed.at[over], b_send.at[1, k], b_recv.at[over], me, pencil - 1)))
        relays.append((goes_high, send(piece, landed.at[under], b_send.at[1, k], b_recv.at[under], me, pencil + 1)))

    def arrival(piece):
        return send(chosen.at[0], landed.at[piece], b_send.at[0, 0], b_recv.at[piece], me, pencil)

    def place(index, piece, value):
        layer, part = divmod(piece, half // 2)
        span = slice(LANES * part, LANES * (part + 1))
        if index == slots:
            mine[layer, :, span] = value
        else:
            held[index, layer, :, span] = value

    blank = jnp.zeros((rows, LANES), jnp.bfloat16)
    for piece in range(groups):
        place(slots, half + piece, outgoing[piece])

    def edge_pieces(present, incoming, pieces, start):
        @pl.when(present)
        def _():
            incoming.wait_recv()
            for piece in pieces:
                place(slots, piece, edges[start + piece - pieces[0]])

        @pl.when(jnp.logical_not(present))
        def _():
            for piece in pieces:
                for index in range(slots + 1):
                    place(index, piece, blank)

    low_pieces = list(range(half))
    high_pieces = list(range(half + groups, 2 * half + groups))
    edge_pieces(has_low, to_high, low_pieces, 0)
    edge_pieces(has_high, to_low, high_pieces, half)
    for copy in weights:
        copy.wait()
    side_sums(fine, mine, matrix, coefs, react, sides, velocity, flux, reflux, produced, spread, state, sums)

    for k, group in enumerate(around):
        if k:
            arrival(half + group).wait_recv()
        for present, copy in relays[2 * k : 2 * k + 2]:
            pl.when(present)(copy.start)
    for piece in range(groups):
        for o in range(slots):
            place(o, half + piece, landed[half + piece, o])
    for present, pieces in ((has_low, low_pieces), (has_high, high_pieces)):

        @pl.when(present)
        def _(pieces=pieces):
            for piece in pieces:
                arrival(piece).wait_recv()
                for o in range(slots):
                    place(o, piece, landed[piece, o])

    for copy in first[1:] + second[1:]:
        copy.wait_send()
    pl.when(has_high)(to_high.wait_send)
    pl.when(has_low)(to_low.wait_send)

    for present, copy in relays:
        pl.when(present)(copy.wait_send)


def route_by_kernel(fine, work, params, coarse_send, flux, patch_owner, velocity, diffusivity, stoich, matrix, sides, own_slots):
    groups = lax.axis_size("gx")
    fields, cells = coarse_send.shape[1:]
    plane = fine * fine // 4
    padded_rows = round_up(fields, 16)
    held_layers = 2 * cells // plane
    piece = (padded_rows, LANES)
    vmem = pl.BlockSpec(memory_space=pltpu.VMEM)
    anywhere = pl.BlockSpec(memory_space=pltpu.HBM)
    dma = pltpu.SemaphoreType.DMA
    bf16 = jnp.bfloat16
    tables, table = prepared(fields)
    return pl.pallas_call(
        functools.partial(route_kernel, fine),
        out_shape=(
            pltpu.VMEM((own_slots, held_layers, padded_rows, plane), bf16),
            pltpu.VMEM(flux.shape, jnp.float32),
        )
        + tuple(pltpu.VMEM(t.shape, t.dtype) for t in tables)
        + (pltpu.VMEM(matrix.shape, bf16),),
        in_specs=[anywhere] * 8,
        out_specs=(vmem,) * 5,
        scratch_shapes=table
        + work
        + [
            pltpu.VMEM((2 * cells // plane, round_up(fields, 8), fine * fine), jnp.float32),
            pltpu.VMEM((held_layers, padded_rows, plane), bf16),
            pltpu.SMEM(patch_owner.shape, jnp.int32),
            pltpu.SMEM(velocity.shape, jnp.float32),
            pltpu.VMEM((fields, cells), bf16),
            pltpu.VMEM(diffusivity.shape, jnp.float32),
            pltpu.VMEM(stoich.shape, jnp.float32),
            pltpu.VMEM(flux.shape, jnp.float32),
            pltpu.VMEM(sides.shape, bf16),
            dma((8,)),
            pltpu.VMEM((padded_rows, cells), jnp.float32),
            pltpu.VMEM((groups,) + piece, bf16),
            pltpu.VMEM((groups,) + piece, bf16),
            pltpu.VMEM((groups + 1,) + piece, bf16),
            pltpu.VMEM((groups, own_slots) + piece, bf16),
            pltpu.VMEM((2 * groups, own_slots) + piece, bf16),
            dma((groups,)),
            dma((groups,)),
            dma((2,)),
            dma((2,)),
            dma((2, groups)),
            dma((2 * groups,)),
        ],
        compiler_params=params(collective_id=0, has_side_effects=True),
        name="route",
    )(*(
        pltpu.with_memory_space_constraint(x, pltpu.HBM)
        for x in (patch_owner, velocity, coarse_send[0], diffusivity, stoich, flux, matrix, sides)
    ))


def side_kernel(fine, velocity, coarse, matrix, diffusivity, stoich, sides, flux, out, coefs, react, table, produced, spread, state, sums):
    prepare(velocity, diffusivity, stoich, coefs, react, table)
    side_sums(fine, coarse, matrix, coefs, react, sides, velocity, flux, out, produced, spread, state, sums)


def route_by_gather(coarse_send, patch_owner, own_slots, padded_rows, plane):
    pencils = lax.axis_size("gy")
    fields, cells = coarse_send.shape[1:]
    my_slots = lax.axis_index("gx") * own_slots + jnp.arange(own_slots, dtype=jnp.int32)
    chooser = (my_slots[:, None] == patch_owner[None, :]).astype(jnp.bfloat16)
    owned = jnp.einsum(
        "oq,qfc->ofc", chooser, lax.all_gather(coarse_send, "gx", axis=0, tiled=True),
        preferred_element_type=jnp.float32,
    ).astype(jnp.bfloat16)
    both = jnp.concatenate([owned, coarse_send], 0)
    forward = [(i, i + 1) for i in range(pencils - 1)]
    backward = [(i + 1, i) for i in range(pencils - 1)]
    below = lax.ppermute(both[:, :, -2 * plane:], "gy", forward)
    above = lax.ppermute(both[:, :, : 2 * plane], "gy", backward)
    held = jnp.concatenate([below, both, above], 2)
    held = jnp.pad(held, ((0, 0), (0, padded_rows - fields), (0, 0)))
    return held.reshape(-1, padded_rows, cells // plane + 4, plane).transpose(0, 2, 1, 3)


def shards(coarse_send, coarse_flux, patch_owner, velocity, diffusivity, stoich):
    send_slots, fields, layer_cells = coarse_send.shape
    pencils = lax.axis_size("gy")
    edge = round((layer_cells * pencils) ** (1.0 / 3.0))
    fine, plane = 2 * edge, edge * edge
    layers = layer_cells // plane
    own_slots = 2 * send_slots
    rows, padded_rows = round_up(fields, 8), round_up(fields, 16)
    width = fine * fine
    deep = 2 * layers

    matrix = jnp.asarray(refine_matrix(edge), jnp.bfloat16)
    sides = jnp.asarray(side_matrix(edge), jnp.bfloat16)
    diffusivity = diffusivity.reshape(1, fields)
    fluxes = coarse_flux.reshape(send_slots, fields, -1, LANES)
    vmem = pl.BlockSpec(memory_space=pltpu.VMEM)
    smem = pl.BlockSpec(memory_space=pltpu.SMEM)
    work = [
        pltpu.VMEM((rows, width), jnp.float32),
        pltpu.VMEM(((layers + 4) * padded_rows, 2 * width), jnp.float32),
        pltpu.VMEM((deep + 4, rows, width), jnp.float32),
    ]
    params = functools.partial(pltpu.CompilerParams, vmem_limit_bytes=48 * 1024 * 1024)

    fits = send_slots == 1 and lax.axis_size("gx") * LANES == layer_cells and layers == 4 and plane == 2 * LANES
    if fits:
        held, reflux, coefs, react, matrix = route_by_kernel(
            fine, work, params, coarse_send, fluxes[0], patch_owner, velocity, diffusivity, stoich, matrix, sides, own_slots
        )
        reflux = reflux[None]
    else:
        held = route_by_gather(coarse_send, patch_owner, own_slots, padded_rows, plane)
        tables, table = prepared(fields)
        reflux = []
        for i in range(send_slots):
            one, coefs, react = pl.pallas_call(
                functools.partial(side_kernel, fine),
                out_shape=(jax.ShapeDtypeStruct(fluxes.shape[1:], jnp.float32),) + tables,
                in_specs=[smem] + [vmem] * 6,
                out_specs=(vmem,) * 3,
                scratch_shapes=table + work + [pltpu.VMEM((deep, rows, width), jnp.float32)],
                compiler_params=params(),
                name="sides",
            )(velocity, held[own_slots + i], matrix, diffusivity, stoich, sides, fluxes[i])
            reflux.append(one)
        reflux = jnp.stack(reflux)
        held = held[:own_slots]
    anywhere = pl.BlockSpec(memory_space=pl.ANY)
    state, reflux = pl.pallas_call(
        functools.partial(fine_kernel, fine),
        out_shape=(
            jax.ShapeDtypeStruct((fields, deep, own_slots * width // LANES, LANES), jnp.float32),
            jax.ShapeDtypeStruct(reflux.shape, jnp.float32),
        ),
        in_specs=[vmem] * 5,
        out_specs=(anywhere, anywhere),
        scratch_shapes=work[1:]
        + [
            pltpu.VMEM((deep + 2, rows, width), jnp.float32),
            pltpu.VMEM((deep, fields, own_slots * width // LANES, LANES), jnp.float32),
            pltpu.SemaphoreType.DMA((deep,)),
            pltpu.SemaphoreType.DMA((1,)),
        ],
        compiler_params=params(),
        name="fine",
    )(held, matrix, coefs, react, reflux)
    state = state.reshape(fields, deep * width // LANES, own_slots, LANES).transpose(2, 0, 1, 3)
    return state.reshape(own_slots, fields, deep * width), reflux.reshape(send_slots, fields, -1)


def solution(mesh):
    placed = (P("gx", None, "gy"), P("gx", None, "gy"), P(), P(), P(), P())
    return jax.shard_map(
        shards,
        mesh=mesh,
        in_specs=placed,
        out_specs=(P("gx", None, "gy"), P("gx", None, "gy")),
        check_vma=False,
    )
```

```python
import functools

import jax
import jax.numpy as jnp
import numpy as np
from jax import lax
from jax.experimental import pallas as pl
from jax.experimental.pallas import tpu as pltpu
from jax.sharding import PartitionSpec as P

time_step = 0.25
LANES = 128


def round_up(count, step):
    return -(-count // step) * step


def lane_groups(fine):
    return LANES // fine, fine * fine // LANES


def planes_to_tiles(columns, fine):
    groups, tiles = lane_groups(fine)
    return columns.reshape(-1, groups, tiles, fine).transpose(0, 2, 1, 3)


def refine_matrix(edge):
    fine = 2 * edge
    copy_1d = np.zeros((edge, fine), np.float32)
    slope_1d = np.zeros((edge, fine), np.float32)
    for j in range(fine):
        i, sign = j // 2, (j % 2 - 0.5) * 0.5
        copy_1d[i, j] = 1.0
        low, high = max(i - 1, 0), min(i + 1, edge - 1)
        scale = sign * (0.5 if high - low == 2 else 1.0)
        slope_1d[high, j] += scale
        slope_1d[low, j] -= scale
    copies = np.einsum("ab,cd->acbd", copy_1d, copy_1d)
    planar = copies + np.einsum("ab,cd->acbd", copy_1d, slope_1d) + np.einsum("ab,cd->acbd", slope_1d, copy_1d)
    planar = planes_to_tiles(planar, fine).reshape(edge * edge, -1)
    copies = planes_to_tiles(copies, fine)[:, ::2].reshape(edge * edge, -1)
    shifts = np.concatenate([np.eye(LANES, k=-1), np.eye(LANES, k=1)], 1)
    shifts = np.tile(shifts, (edge * edge // LANES, 1)) * (np.arange(edge * edge) < 2 * LANES)[:, None]
    return np.concatenate([planar, copies * 0.125, shifts], 1)


def side_matrix(edge):
    fine = 2 * edge
    pick = np.zeros((fine, fine, 4, edge), np.float32)
    for along in range(fine):
        pick[along, 0, 0, along // 2] = 1.0
        pick[along, fine - 1, 1, along // 2] = 1.0
        pick[0, along, 2, along // 2] = 1.0
        pick[fine - 1, along, 3, along // 2] = 1.0
    pick = planes_to_tiles(pick.reshape(fine * fine, 4 * edge).T, fine).reshape(4 * edge, -1).T
    return np.tile(pick, (1, max(1, LANES // (4 * edge))))


def split_halves(values):
    high = values.astype(jnp.bfloat16)
    low = (values - high.astype(jnp.float32)).astype(jnp.bfloat16)
    return high, low


def react_layer(source, index, react, shifts):
    rows, width = source.shape[1:]
    field_rows = react.shape[1] // 3
    cells = source[index]
    rate = 1.0 + jnp.tanh(source[index, 0:1, :])
    high, low = split_halves(jnp.concatenate([cells, jnp.zeros((field_rows - rows, width), jnp.float32)], 0))
    made = rate * jnp.dot(react[...], jnp.concatenate([high, high, low], 0), preferred_element_type=jnp.float32)
    beside = None
    if shifts is not None:
        spans = [slice(LANES * t, LANES * (t + 1)) for t in range(width // LANES)]
        joined = jnp.concatenate([jnp.concatenate([high[:, x], low[:, x]], 1) for x in spans], 0)
        beside = jnp.dot(joined, shifts, preferred_element_type=jnp.float32)
        beside = [beside[field_rows * t : field_rows * t + rows] for t in range(len(spans))]
    return made, beside


def run_layers(source, start, count, coefs, react, fine, use, together, shifts=None, layerwise=False):
    rows = source.shape[1]

    def some(first):
        layers = [first * together + i for i in range(together)]
        groups = range(rows // 8)
        produced = None if layerwise else [react_layer(source, start + layer, react, shifts) for layer in layers]
        order = [(i, g) for i in range(together) for g in groups] if layerwise else [(i, g) for g in groups for i in range(together)]
        for i, group in order:
            band = slice(8 * group, 8 * group + 8)
            held = [coefs[i, band, :] for i in range(coefs.shape[0])]
            if layerwise and group == 0:
                made, beside = react_layer(source, start + layers[i], react, shifts)
            elif not layerwise:
                made, beside = produced[i]
            use(layers[i], group, step_group(source, start + layers[i], band, held, made, beside, fine))

    if count == together:
        some(0)
    else:
        pl.loop(0, count // together)(some)


def step_group(source, index, band, coefs, produced, beside, fine):
    tiles = source.shape[2] // LANES
    cells = [source[index, band, LANES * t : LANES * (t + 1)] for t in range(tiles)]
    across = []
    for t in range(tiles):
        span = slice(LANES * t, LANES * (t + 1))
        c = cells[t]
        first, last = t == 0, t == tiles - 1
        if beside is None:
            x_high, x_low = pltpu.roll(c, LANES - 1, 1), pltpu.roll(c, 1, 1)
        else:
            x_high, x_low = beside[t][band, :LANES], beside[t][band, LANES:]
        y_high = pltpu.roll(cells[0], LANES - fine, 1) if last else cells[t + 1]
        y_low = pltpu.roll(cells[-1], fine, 1) if first else cells[t - 1]
        total = coefs[0] * x_high + coefs[1] * x_low
        total += coefs[9 if last else 2] * y_high + coefs[10 if first else 3] * y_low
        total += coefs[4] * source[index + 1, band, span] + coefs[5] * source[index - 1, band, span]
        total += coefs[7 if first else 8 if last else 6] * c
        across.append(total + produced[band, span])
    return across


def to_planes(across, fine):
    groups, tiles = lane_groups(fine)
    group = lax.broadcasted_iota(jnp.int32, (8, LANES), 1) // fine
    masks = [lax.rem(group // step, 2) == 0 for step in (1, 2)]
    out = [None] * tiles
    for first in range(0, tiles, groups):
        turned = [pltpu.roll(c, j * fine, 1) if j else c for j, c in enumerate(across[first : first + groups])]
        for a in range(groups):
            order = [turned[(g - a) % groups] for g in range(groups)]
            mixed = order[0]
            if groups == 4:
                mixed = jnp.where(masks[1], jnp.where(masks[0], *order[:2]), jnp.where(masks[0], *order[2:]))
            else:
                for g in range(1, groups):
                    mixed = jnp.where(group == g, order[g], mixed)
            out[a * (tiles // groups) + first // groups] = pltpu.roll(mixed, LANES - a * fine, 1) if a else mixed
    return out


def store_group(target, index, group, across):
    for t, value in enumerate(across):
        target[index, 8 * group : 8 * group + 8, LANES * t : LANES * (t + 1)] = value


def fill_layers(coarse, matrix, state, at_bottom, at_top):
    held, padded_rows, cells = coarse.shape
    rows, width = state.shape[1:]
    flat = coarse[...].reshape(held * padded_rows, cells)
    inner = flat[padded_rows:-padded_rows]
    chunk = 2 * LANES
    for part in range(width // 2 // chunk):
        spread = jnp.dot(flat, matrix[:, width + part * chunk : width + (part + 1) * chunk], preferred_element_type=jnp.float32)
        copies = [spread[i * padded_rows : i * padded_rows + rows] for i in range(held)]
        copies[1] = jnp.where(at_bottom, 2.0 * copies[2] - copies[3], copies[1])
        copies[-2] = jnp.where(at_top, 2.0 * copies[-3] - copies[-4], copies[-2])
        slopes = [copies[i + 1] - copies[i - 1] for i in range(1, held - 1)]
        for t in range(2):
            start = part * 2 * chunk + t * chunk
            planar = jnp.dot(inner, matrix[:, start : start + chunk], preferred_element_type=jnp.float32)
            slope = [jnp.concatenate([s[:, t * LANES : (t + 1) * LANES]] * 2, 1) for s in slopes]
            layers = []
            for i in range(held - 2):
                middle = planar[i * padded_rows : i * padded_rows + rows]
                layers += [middle - slope[i], middle + slope[i]]
            layers[1] = jnp.where(at_bottom, layers[2], layers[1])
            layers[-2] = jnp.where(at_top, layers[-3], layers[-2])
            for i, layer in enumerate(layers):
                state[i, :, start : start + chunk] = layer


def pencil_ends():
    pencil = lax.axis_index("gy")
    return pencil == 0, pencil == lax.axis_size("gy") - 1


def prepare(velocity, diffusivity, stoich, coefs, react, table, fine):
    fields = stoich.shape[0]
    rows = coefs.shape[1]
    part = react.shape[1] // 3
    table[...] = jnp.zeros(table.shape, jnp.float32)
    table[:fields, :fields] = stoich[...] * (time_step * 0.5)
    scaled = table[...]
    high = scaled.astype(jnp.bfloat16).astype(jnp.float32)
    low = scaled - high
    joined = high + pltpu.roll(low, part, 1) + pltpu.roll(high, 2 * part, 1)
    react[...] = joined[:, : 3 * part].astype(jnp.bfloat16)
    table[...] = jnp.zeros(table.shape, jnp.float32)
    table[0:1, :fields] = diffusivity[...]
    shape = (rows, LANES)
    lane = lax.broadcasted_iota(jnp.int32, shape, 1)
    diagonal = lax.broadcasted_iota(jnp.int32, shape, 0) == lane
    line = jnp.broadcast_to(table[0:1, :LANES], shape)
    column = jnp.sum(jnp.where(diagonal, line, 0.0), 1, keepdims=True)
    diffuse = jnp.broadcast_to(column, shape)
    highs = [(diffuse - velocity[dim] * 0.5) * time_step for dim in range(3)]
    lows = [(diffuse + velocity[dim] * 0.5) * time_step for dim in range(3)]
    x = lax.rem(lane, fine)
    first_x, last_x = x == 0, x == fine - 1
    first_y, last_y = lane < fine, lane >= LANES - fine
    zero = jnp.zeros(shape, jnp.float32)
    center = 1.0 - 6.0 * time_step * diffuse
    center += jnp.where(last_x, highs[0], zero) + jnp.where(first_x, lows[0], zero)
    values = [
        jnp.where(last_x, zero, highs[0]), jnp.where(first_x, zero, lows[0]), highs[1], lows[1], highs[2], lows[2],
        center, center + jnp.where(first_y, lows[1], zero), center + jnp.where(last_y, highs[1], zero),
        jnp.where(last_y, zero, highs[1]), jnp.where(first_y, zero, lows[1]),
    ]
    for i, value in enumerate(values):
        coefs[i] = value


def prepared(fields):
    rows, padded_rows = round_up(fields, 8), round_up(fields, 16)
    return (
        jax.ShapeDtypeStruct((11, rows, LANES), jnp.float32),
        jax.ShapeDtypeStruct((rows, 3 * padded_rows), jnp.bfloat16),
    ), [pltpu.VMEM((rows, round_up(3 * padded_rows, LANES)), jnp.float32)]


def fine_kernel(fine, coarse, matrix, coefs, react, reflux, out, reflux_out, state, middle, ready, sems, reflux_sem):
    reflux_copy = pltpu.make_async_copy(reflux, reflux_out, reflux_sem.at[0])
    reflux_copy.start()
    at_bottom, at_top = pencil_ends()
    slots = out.shape[2] * LANES // state.shape[2]
    shifts = matrix[:, -2 * LANES :]
    fields = out.shape[0]
    layers = out.shape[1]
    step = out.shape[2]

    def copy_out(layer, group):
        some = pl.ds(8 * group, min(8, fields - 8 * group))
        return pltpu.make_async_copy(ready.at[layer, some], out.at[some, layer], sems.at[layer, group])

    for slot in range(slots):
        fill_layers(coarse.at[slot], matrix, state, at_bottom, at_top)

        def to_middle(layer, group, across):
            store_group(middle, layer, group, across)

        run_layers(state, 1, layers + 2, coefs, react, fine, to_middle, (layers + 2) // 2)

        @pl.when(at_bottom)
        def _():
            middle[0] = middle[1]

        @pl.when(at_top)
        def _():
            middle[layers + 1] = middle[layers]

        def to_output(layer, group, across):
            low, high = 8 * group, min(8 * group + 8, fields)
            halves = []
            for t, value in enumerate(across):
                span = slice(LANES * t, LANES * (t + 1))
                halves.append((value + state[layer + 2, low : low + 8, span]) * 0.5)
            lines = ready.at[layer].reshape(fields * step, LANES)
            for t, value in enumerate(to_planes(halves, fine)):
                lines[pl.ds(low * step + t * slots + slot, high - low, stride=step), :] = value[: high - low]
            if slot == slots - 1:
                copy_out(layer, group).start()

        run_layers(middle, 1, layers, coefs, react, fine, to_output, layers, shifts, True)

    for layer in range(layers):
        for group in range(sems.shape[1]):
            copy_out(layer, group).wait()
    reflux_copy.wait()


def side_sums(fine, coarse, matrix, coefs, react, sides, velocity, flux, out, state, sums):
    at_bottom, at_top = pencil_ends()
    fields = out.shape[0]
    rows, width = state.shape[1:]
    layers = state.shape[0] - 4
    fill_layers(coarse, matrix, state, at_bottom, at_top)

    def to_sums(layer, group, across):
        band = slice(8 * group, 8 * group + 8)
        for t, value in enumerate(across):
            span = slice(LANES * t, LANES * (t + 1))
            sums[layer, band, span] = value + state[layer + 2, band, span]

    run_layers(state, 2, layers, coefs, react, fine, to_sums, 2)
    pads = jnp.zeros((round_up(rows, 16) - rows, width), jnp.float32)
    halves = []
    for pair in range(layers // 2):
        high, low = split_halves(jnp.concatenate([sums[2 * pair] + sums[2 * pair + 1], pads], 0))
        halves += [high, low]
    picked = jnp.dot(jnp.concatenate(halves, 0), sides[...], preferred_element_type=jnp.float32)
    step = rows + pads.shape[0]
    each = [
        picked[2 * step * i : 2 * step * i + rows] + picked[2 * step * i + step : 2 * step * i + step + rows]
        for i in range(layers // 2)
    ]
    span = sides.shape[1]
    per_tile = span // (fine * 2)
    lane = lax.broadcasted_iota(jnp.int32, (rows, span), 1)
    for tile in range(len(each) // per_tile):
        value = each[tile * per_tile]
        for i in range(1, per_tile):
            value = jnp.where(lane >= i * fine * 2, each[tile * per_tile + i], value)
        along_x = lax.rem(lane, fine * 2) < fine
        value = value * jnp.where(along_x, velocity[0] * 0.125, velocity[1] * 0.125)
        out[:, tile, :] = value[:fields] - flux[:, tile, :]


def route_kernel(
    fine, owner_hbm, velocity_hbm, own_hbm, diffusivity_hbm, stoich_hbm, flux_hbm, matrix_hbm, sides_hbm,
    held, reflux, coefs, react, matrix, table, state, sums, mine,
    owner, velocity, own, diffusivity, stoich, flux, sides, w_sems,
    outgoing, edges, arrived, chosen, landed, a_send, a_recv, h_send, h_recv, b_send, b_recv,
):
    me, pencil = lax.axis_index("gx"), lax.axis_index("gy")
    groups, pencils = lax.axis_size("gx"), lax.axis_size("gy")
    fields = own.shape[0]
    rows, sent = outgoing.shape[1], round_up(fields, 8)
    half = groups // 2
    pairs = (
        (own_hbm, own), (owner_hbm, owner), (velocity_hbm, velocity), (diffusivity_hbm, diffusivity),
        (stoich_hbm, stoich), (flux_hbm, flux), (matrix_hbm, matrix), (sides_hbm, sides),
    )
    fetches = [pltpu.make_async_copy(source, target, w_sems.at[i]) for i, (source, target) in enumerate(pairs)]
    for copy in fetches:
        copy.start()
    own_in, owner_in, small_in, weights = fetches[0], fetches[1], fetches[2:5], fetches[5:]
    slots = chosen.shape[1]
    has_low, has_high = pencil > 0, pencil < pencils - 1
    around = [lax.rem(me + k, groups) for k in range(groups)]

    barrier = pltpu.get_barrier_semaphore()

    def greet(group, to):
        pl.semaphore_signal(barrier, inc=1, device_id=(group, to), device_id_type=pl.DeviceIdType.MESH)

    for group in around[1:]:
        greet(group, pencil)

    @pl.when(has_low)
    def _():
        greet(me, pencil - 1)

    @pl.when(has_high)
    def _():
        greet(me, pencil + 1)

    own_in.wait()
    for piece in range(groups):
        outgoing[piece, :fields] = own[:, LANES * piece : LANES * (piece + 1)]
        outgoing[piece, fields:] = jnp.zeros((rows - fields, LANES), jnp.bfloat16)
    arrived[me] = outgoing[me]
    arrived[groups] = jnp.zeros(arrived.shape[1:], jnp.bfloat16)

    near = groups - 1
    pl.semaphore_wait(barrier, near + (has_low.astype(jnp.int32) + has_high.astype(jnp.int32)))

    def send(src, dst, out_sem, in_sem, group, to):
        return pltpu.make_async_remote_copy(
            src_ref=src, dst_ref=dst, send_sem=out_sem, recv_sem=in_sem,
            device_id=(group, to), device_id_type=pl.DeviceIdType.MESH,
        )

    first = [
        send(outgoing.at[group, :sent], arrived.at[me, :sent], a_send.at[k], a_recv.at[me], group, pencil)
        for k, group in enumerate(around)
    ]
    to_high = send(outgoing.at[half:, :sent], edges.at[:half, :sent], h_send.at[0], h_recv.at[0], me, pencil + 1)
    to_low = send(outgoing.at[:half, :sent], edges.at[half:, :sent], h_send.at[1], h_recv.at[1], me, pencil - 1)
    for copy in first[1:]:
        copy.start()
    pl.when(has_high)(to_high.start)
    pl.when(has_low)(to_low.start)
    owner_in.wait()
    sources = []
    for group in around:
        for o in range(slots):
            slot = group * slots + o
            source = jnp.int32(groups)
            for q in range(groups):
                source = jnp.where(owner[q] == slot, q, source)
            sources.append(source)

    for copy in small_in:
        copy.wait()
    prepare(velocity, diffusivity, stoich, coefs, react, table, fine)
    for group in around[1:]:
        send(outgoing.at[group, :sent], arrived.at[group, :sent], a_send.at[0], a_recv.at[group], group, pencil).wait_recv()

    for k, group in enumerate(around):
        for o in range(slots):
            chosen[group, o, :sent] = arrived[sources[k * slots + o], :sent]
    landed[half + me, :, :sent] = chosen[me, :, :sent]

    second = [
        send(chosen.at[group, :, :sent], landed.at[half + me, :, :sent], b_send.at[0, k], b_recv.at[half + me], group, pencil)
        for k, group in enumerate(around)
    ]
    for copy in second[1:]:
        copy.start()

    relays = []
    for k, group in enumerate(around):
        piece = landed.at[half + group, :, :sent]
        goes_low = jnp.logical_and(has_low, group < half)
        goes_high = jnp.logical_and(has_high, group >= half)
        over, under = half + groups + group, lax.rem(group + half, groups)
        relays.append((goes_low, send(piece, landed.at[over, :, :sent], b_send.at[1, k], b_recv.at[over], me, pencil - 1)))
        relays.append((goes_high, send(piece, landed.at[under, :, :sent], b_send.at[1, k], b_recv.at[under], me, pencil + 1)))

    def arrival(piece):
        return send(chosen.at[0, :, :sent], landed.at[piece, :, :sent], b_send.at[0, 0], b_recv.at[piece], me, pencil)

    def place(index, piece, value):
        layer, part = divmod(piece, half // 2)
        span = slice(LANES * part, LANES * (part + 1))
        if index == slots:
            mine[layer, : value.shape[0], span] = value
        else:
            held[index, layer, : value.shape[0], span] = value

    blank = jnp.zeros((rows, LANES), jnp.bfloat16)
    for layer in range(mine.shape[0]):
        for index in range(slots):
            held[index, layer, sent:, :] = jnp.zeros((rows - sent, held.shape[3]), jnp.bfloat16)
        mine[layer, sent:, :] = jnp.zeros((rows - sent, held.shape[3]), jnp.bfloat16)
    for piece in range(groups):
        place(slots, half + piece, outgoing[piece])

    def edge_pieces(present, incoming, pieces, start):
        @pl.when(present)
        def _():
            incoming.wait_recv()
            for piece in pieces:
                place(slots, piece, edges[start + piece - pieces[0], :sent])

        @pl.when(jnp.logical_not(present))
        def _():
            for piece in pieces:
                for index in range(slots + 1):
                    place(index, piece, blank)

    low_pieces = list(range(half))
    high_pieces = list(range(half + groups, 2 * half + groups))
    edge_pieces(has_low, to_high, low_pieces, 0)
    edge_pieces(has_high, to_low, high_pieces, half)
    for copy in weights:
        copy.wait()
    side_sums(fine, mine, matrix, coefs, react, sides, velocity, flux, reflux, state, sums)

    for k, group in enumerate(around):
        if k:
            arrival(half + group).wait_recv()
        for present, copy in relays[2 * k : 2 * k + 2]:
            pl.when(present)(copy.start)
    for piece in range(groups):
        for o in range(slots):
            place(o, half + piece, landed[half + piece, o, :sent])
    for present, pieces in ((has_low, low_pieces), (has_high, high_pieces)):

        @pl.when(present)
        def _(pieces=pieces):
            for piece in pieces:
                arrival(piece).wait_recv()
                for o in range(slots):
                    place(o, piece, landed[piece, o, :sent])

    for copy in first[1:] + second[1:]:
        copy.wait_send()
    pl.when(has_high)(to_high.wait_send)
    pl.when(has_low)(to_low.wait_send)

    for present, copy in relays:
        pl.when(present)(copy.wait_send)


def route_by_kernel(fine, work, params, coarse_send, flux, patch_owner, velocity, diffusivity, stoich, matrix, sides, own_slots):
    groups = lax.axis_size("gx")
    fields, cells = coarse_send.shape[1:]
    plane = fine * fine // 4
    padded_rows = round_up(fields, 16)
    held_layers = 2 * cells // plane
    piece = (padded_rows, LANES)
    vmem = pl.BlockSpec(memory_space=pltpu.VMEM)
    anywhere = pl.BlockSpec(memory_space=pltpu.HBM)
    dma = pltpu.SemaphoreType.DMA
    bf16 = jnp.bfloat16
    tables, table = prepared(fields)
    return pl.pallas_call(
        functools.partial(route_kernel, fine),
        out_shape=(
            pltpu.VMEM((own_slots, held_layers, padded_rows, plane), bf16),
            pltpu.VMEM(flux.shape, jnp.float32),
        )
        + tuple(pltpu.VMEM(t.shape, t.dtype) for t in tables)
        + (pltpu.VMEM(matrix.shape, bf16),),
        in_specs=[anywhere] * 8,
        out_specs=(vmem,) * 5,
        scratch_shapes=table
        + work
        + [
            pltpu.VMEM((2 * cells // plane, round_up(fields, 8), fine * fine), jnp.float32),
            pltpu.VMEM((held_layers, padded_rows, plane), bf16),
            pltpu.SMEM(patch_owner.shape, jnp.int32),
            pltpu.SMEM(velocity.shape, jnp.float32),
            pltpu.VMEM((fields, cells), bf16),
            pltpu.VMEM(diffusivity.shape, jnp.float32),
            pltpu.VMEM(stoich.shape, jnp.float32),
            pltpu.VMEM(flux.shape, jnp.float32),
            pltpu.VMEM(sides.shape, bf16),
            dma((8,)),
            pltpu.VMEM((groups,) + piece, bf16),
            pltpu.VMEM((groups,) + piece, bf16),
            pltpu.VMEM((groups + 1,) + piece, bf16),
            pltpu.VMEM((groups, own_slots) + piece, bf16),
            pltpu.VMEM((2 * groups, own_slots) + piece, bf16),
            dma((groups,)),
            dma((groups,)),
            dma((2,)),
            dma((2,)),
            dma((2, groups)),
            dma((2 * groups,)),
        ],
        compiler_params=params(collective_id=0, has_side_effects=True),
        name="route",
    )(*(
        pltpu.with_memory_space_constraint(x, pltpu.HBM)
        for x in (patch_owner, velocity, coarse_send[0], diffusivity, stoich, flux, matrix, sides)
    ))


def side_kernel(fine, velocity, coarse, matrix, diffusivity, stoich, sides, flux, out, coefs, react, table, state, sums):
    prepare(velocity, diffusivity, stoich, coefs, react, table, fine)
    side_sums(fine, coarse, matrix, coefs, react, sides, velocity, flux, out, state, sums)


def route_by_gather(coarse_send, patch_owner, own_slots, padded_rows, plane):
    pencils = lax.axis_size("gy")
    fields, cells = coarse_send.shape[1:]
    my_slots = lax.axis_index("gx") * own_slots + jnp.arange(own_slots, dtype=jnp.int32)
    chooser = (my_slots[:, None] == patch_owner[None, :]).astype(jnp.bfloat16)
    owned = jnp.einsum(
        "oq,qfc->ofc", chooser, lax.all_gather(coarse_send, "gx", axis=0, tiled=True),
        preferred_element_type=jnp.float32,
    ).astype(jnp.bfloat16)
    both = jnp.concatenate([owned, coarse_send], 0)
    forward = [(i, i + 1) for i in range(pencils - 1)]
    backward = [(i + 1, i) for i in range(pencils - 1)]
    below = lax.ppermute(both[:, :, -2 * plane:], "gy", forward)
    above = lax.ppermute(both[:, :, : 2 * plane], "gy", backward)
    held = jnp.concatenate([below, both, above], 2)
    held = jnp.pad(held, ((0, 0), (0, padded_rows - fields), (0, 0)))
    return held.reshape(-1, padded_rows, cells // plane + 4, plane).transpose(0, 2, 1, 3)


def shards(coarse_send, coarse_flux, patch_owner, velocity, diffusivity, stoich):
    send_slots, fields, layer_cells = coarse_send.shape
    pencils = lax.axis_size("gy")
    edge = round((layer_cells * pencils) ** (1.0 / 3.0))
    fine, plane = 2 * edge, edge * edge
    layers = layer_cells // plane
    own_slots = 2 * send_slots
    rows, padded_rows = round_up(fields, 8), round_up(fields, 16)
    width = fine * fine
    deep = 2 * layers

    matrix = jnp.asarray(refine_matrix(edge), jnp.bfloat16)
    sides = jnp.asarray(side_matrix(edge), jnp.bfloat16)
    diffusivity = diffusivity.reshape(1, fields)
    fluxes = coarse_flux.reshape(send_slots, fields, -1, LANES)
    vmem = pl.BlockSpec(memory_space=pltpu.VMEM)
    smem = pl.BlockSpec(memory_space=pltpu.SMEM)
    work = [pltpu.VMEM((deep + 4, rows, width), jnp.float32)]
    params = functools.partial(pltpu.CompilerParams, vmem_limit_bytes=48 * 1024 * 1024)

    fits = send_slots == 1 and lax.axis_size("gx") * LANES == layer_cells and layers == 4 and plane == 2 * LANES
    if fits:
        held, reflux, coefs, react, matrix = route_by_kernel(
            fine, work, params, coarse_send, fluxes[0], patch_owner, velocity, diffusivity, stoich, matrix, sides, own_slots
        )
        reflux = reflux[None]
    else:
        held = route_by_gather(coarse_send, patch_owner, own_slots, padded_rows, plane)
        tables, table = prepared(fields)
        reflux = []
        for i in range(send_slots):
            one, coefs, react = pl.pallas_call(
                functools.partial(side_kernel, fine),
                out_shape=(jax.ShapeDtypeStruct(fluxes.shape[1:], jnp.float32),) + tables,
                in_specs=[smem] + [vmem] * 6,
                out_specs=(vmem,) * 3,
                scratch_shapes=table + work + [pltpu.VMEM((deep, rows, width), jnp.float32)],
                compiler_params=params(),
                name="sides",
            )(velocity, held[own_slots + i], matrix, diffusivity, stoich, sides, fluxes[i])
            reflux.append(one)
        reflux = jnp.stack(reflux)
        held = held[:own_slots]
    anywhere = pl.BlockSpec(memory_space=pl.ANY)
    state, reflux = pl.pallas_call(
        functools.partial(fine_kernel, fine),
        out_shape=(
            jax.ShapeDtypeStruct((fields, deep, own_slots * width // LANES, LANES), jnp.float32),
            jax.ShapeDtypeStruct(reflux.shape, jnp.float32),
        ),
        in_specs=[vmem] * 5,
        out_specs=(anywhere, anywhere),
        scratch_shapes=work
        + [
            pltpu.VMEM((deep + 2, rows, width), jnp.float32),
            pltpu.VMEM((deep, fields, own_slots * width // LANES, LANES), jnp.float32),
            pltpu.SemaphoreType.DMA((deep, rows // 8)),
            pltpu.SemaphoreType.DMA((1,)),
        ],
        compiler_params=params(),
        name="fine",
    )(held, matrix, coefs, react, reflux)
    state = state.reshape(fields, deep * width // LANES, own_slots, LANES).transpose(2, 0, 1, 3)
    return state.reshape(own_slots, fields, deep * width), reflux.reshape(send_slots, fields, -1)


def solution(mesh):
    placed = (P("gx", None, "gy"), P("gx", None, "gy"), P(), P(), P(), P())
    return jax.shard_map(
        shards,
        mesh=mesh,
        in_specs=placed,
        out_specs=(P("gx", None, "gy"), P("gx", None, "gy")),
        check_vma=False,
    )
```

```python
import functools

import jax
import jax.numpy as jnp
import numpy as np
from jax import lax
from jax.experimental import pallas as pl
from jax.experimental.pallas import tpu as pltpu
from jax.sharding import PartitionSpec as P

time_step = 0.25
LANES = 128


def round_up(count, step):
    return -(-count // step) * step


def lane_groups(fine):
    return LANES // fine, fine * fine // LANES


def planes_to_tiles(columns, fine):
    groups, tiles = lane_groups(fine)
    return columns.reshape(-1, groups, tiles, fine).transpose(0, 2, 1, 3)


def refine_matrix(edge):
    fine = 2 * edge
    copy_1d = np.zeros((edge, fine), np.float32)
    slope_1d = np.zeros((edge, fine), np.float32)
    for j in range(fine):
        i, sign = j // 2, (j % 2 - 0.5) * 0.5
        copy_1d[i, j] = 1.0
        low, high = max(i - 1, 0), min(i + 1, edge - 1)
        scale = sign * (0.5 if high - low == 2 else 1.0)
        slope_1d[high, j] += scale
        slope_1d[low, j] -= scale
    copies = np.einsum("ab,cd->acbd", copy_1d, copy_1d)
    planar = copies + np.einsum("ab,cd->acbd", copy_1d, slope_1d) + np.einsum("ab,cd->acbd", slope_1d, copy_1d)
    planar = planes_to_tiles(planar, fine).reshape(edge * edge, -1)
    copies = planes_to_tiles(copies, fine)[:, ::2].reshape(edge * edge, -1)
    shifts = np.concatenate([np.eye(LANES, k=-1), np.eye(LANES, k=1)], 1)
    shifts = np.tile(shifts, (edge * edge // LANES, 1)) * (np.arange(edge * edge) < 2 * LANES)[:, None]
    return np.concatenate([planar, copies * 0.125, shifts], 1)


def side_matrix(edge):
    fine = 2 * edge
    pick = np.zeros((fine, fine, 4, edge), np.float32)
    for along in range(fine):
        pick[along, 0, 0, along // 2] = 1.0
        pick[along, fine - 1, 1, along // 2] = 1.0
        pick[0, along, 2, along // 2] = 1.0
        pick[fine - 1, along, 3, along // 2] = 1.0
    pick = planes_to_tiles(pick.reshape(fine * fine, 4 * edge).T, fine).reshape(4 * edge, -1).T
    return np.tile(pick, (1, max(1, LANES // (4 * edge))))


def split_halves(values):
    high = values.astype(jnp.bfloat16)
    low = (values - high.astype(jnp.float32)).astype(jnp.bfloat16)
    return high, low


def react_layer(source, index, react, shifts):
    rows, width = source.shape[1:]
    field_rows = react.shape[1] // 3
    cells = source[index]
    rate = 1.0 + jnp.tanh(source[index, 0:1, :])
    high, low = split_halves(jnp.concatenate([cells, jnp.zeros((field_rows - rows, width), jnp.float32)], 0))
    made = rate * jnp.dot(react[...], jnp.concatenate([high, high, low], 0), preferred_element_type=jnp.float32)
    beside = None
    if shifts is not None:
        spans = [slice(LANES * t, LANES * (t + 1)) for t in range(width // LANES)]
        joined = jnp.concatenate([jnp.concatenate([high[:, x], low[:, x]], 1) for x in spans], 0)
        beside = jnp.dot(joined, shifts, preferred_element_type=jnp.float32)
        beside = [beside[field_rows * t : field_rows * t + rows] for t in range(len(spans))]
    return made, beside


def run_layers(source, start, count, coefs, react, fine, use, together, shifts=None, layerwise=False):
    rows = source.shape[1]

    def some(first):
        layers = [first * together + i for i in range(together)]
        groups = range(rows // 8)
        produced = None if layerwise else [react_layer(source, start + layer, react, shifts) for layer in layers]
        order = [(i, g) for i in range(together) for g in groups] if layerwise else [(i, g) for g in groups for i in range(together)]
        for i, group in order:
            band = slice(8 * group, 8 * group + 8)
            held = [coefs[i, band, :] for i in range(coefs.shape[0])]
            if layerwise and group == 0:
                made, beside = react_layer(source, start + layers[i], react, shifts)
            elif not layerwise:
                made, beside = produced[i]
            use(layers[i], group, step_group(source, start + layers[i], band, held, made, beside, fine))

    if count == together:
        some(0)
    else:
        pl.loop(0, count // together)(some)


def step_group(source, index, band, coefs, produced, beside, fine):
    tiles = source.shape[2] // LANES
    cells = [source[index, band, LANES * t : LANES * (t + 1)] for t in range(tiles)]
    across = []
    for t in range(tiles):
        span = slice(LANES * t, LANES * (t + 1))
        c = cells[t]
        first, last = t == 0, t == tiles - 1
        if beside is None:
            x_high, x_low = pltpu.roll(c, LANES - 1, 1), pltpu.roll(c, 1, 1)
        else:
            x_high, x_low = beside[t][band, :LANES], beside[t][band, LANES:]
        y_high = pltpu.roll(cells[0], LANES - fine, 1) if last else cells[t + 1]
        y_low = pltpu.roll(cells[-1], fine, 1) if first else cells[t - 1]
        total = coefs[0] * x_high + coefs[1] * x_low
        total += coefs[9 if last else 2] * y_high + coefs[10 if first else 3] * y_low
        total += coefs[4] * source[index + 1, band, span] + coefs[5] * source[index - 1, band, span]
        total += coefs[7 if first else 8 if last else 6] * c
        across.append(total + produced[band, span])
    return across


def to_planes(across, fine):
    groups, tiles = lane_groups(fine)
    group = lax.broadcasted_iota(jnp.int32, (8, LANES), 1) // fine
    masks = [lax.rem(group // step, 2) == 0 for step in (1, 2)]
    out = [None] * tiles
    for first in range(0, tiles, groups):
        turned = [pltpu.roll(c, j * fine, 1) if j else c for j, c in enumerate(across[first : first + groups])]
        for a in range(groups):
            order = [turned[(g - a) % groups] for g in range(groups)]
            mixed = order[0]
            if groups == 4:
                mixed = jnp.where(masks[1], jnp.where(masks[0], *order[:2]), jnp.where(masks[0], *order[2:]))
            else:
                for g in range(1, groups):
                    mixed = jnp.where(group == g, order[g], mixed)
            out[a * (tiles // groups) + first // groups] = pltpu.roll(mixed, LANES - a * fine, 1) if a else mixed
    return out


def store_group(target, index, group, across):
    for t, value in enumerate(across):
        target[index, 8 * group : 8 * group + 8, LANES * t : LANES * (t + 1)] = value


def fill_layers(coarse, matrix, state, at_bottom, at_top):
    held, padded_rows, cells = coarse.shape
    rows, width = state.shape[1:]
    flat = coarse[...].reshape(held * padded_rows, cells)
    inner = flat[padded_rows:-padded_rows]
    chunk = 2 * LANES
    for part in range(width // 2 // chunk):
        spread = jnp.dot(flat, matrix[:, width + part * chunk : width + (part + 1) * chunk], preferred_element_type=jnp.float32)
        copies = [spread[i * padded_rows : i * padded_rows + rows] for i in range(held)]
        copies[1] = jnp.where(at_bottom, 2.0 * copies[2] - copies[3], copies[1])
        copies[-2] = jnp.where(at_top, 2.0 * copies[-3] - copies[-4], copies[-2])
        slopes = [copies[i + 1] - copies[i - 1] for i in range(1, held - 1)]
        for t in range(2):
            start = part * 2 * chunk + t * chunk
            planar = jnp.dot(inner, matrix[:, start : start + chunk], preferred_element_type=jnp.float32)
            slope = [jnp.concatenate([s[:, t * LANES : (t + 1) * LANES]] * 2, 1) for s in slopes]
            layers = []
            for i in range(held - 2):
                middle = planar[i * padded_rows : i * padded_rows + rows]
                layers += [middle - slope[i], middle + slope[i]]
            layers[1] = jnp.where(at_bottom, layers[2], layers[1])
            layers[-2] = jnp.where(at_top, layers[-3], layers[-2])
            for i, layer in enumerate(layers):
                state[i, :, start : start + chunk] = layer


def pencil_ends():
    pencil = lax.axis_index("gy")
    return pencil == 0, pencil == lax.axis_size("gy") - 1


def prepare(velocity, diffusivity, stoich, coefs, react, table, fine):
    fields = stoich.shape[0]
    rows = coefs.shape[1]
    part = react.shape[1] // 3
    table[...] = jnp.zeros(table.shape, jnp.float32)
    table[:fields, :fields] = stoich[...] * (time_step * 0.5)
    scaled = table[...]
    high = scaled.astype(jnp.bfloat16).astype(jnp.float32)
    low = scaled - high
    joined = high + pltpu.roll(low, part, 1) + pltpu.roll(high, 2 * part, 1)
    react[...] = joined[:, : 3 * part].astype(jnp.bfloat16)
    table[...] = jnp.zeros(table.shape, jnp.float32)
    table[0:1, :fields] = diffusivity[...]
    shape = (rows, LANES)
    lane = lax.broadcasted_iota(jnp.int32, shape, 1)
    diagonal = lax.broadcasted_iota(jnp.int32, shape, 0) == lane
    line = jnp.broadcast_to(table[0:1, :LANES], shape)
    column = jnp.sum(jnp.where(diagonal, line, 0.0), 1, keepdims=True)
    diffuse = jnp.broadcast_to(column, shape)
    highs = [(diffuse - velocity[dim] * 0.5) * time_step for dim in range(3)]
    lows = [(diffuse + velocity[dim] * 0.5) * time_step for dim in range(3)]
    x = lax.rem(lane, fine)
    first_x, last_x = x == 0, x == fine - 1
    first_y, last_y = lane < fine, lane >= LANES - fine
    zero = jnp.zeros(shape, jnp.float32)
    center = 1.0 - 6.0 * time_step * diffuse
    center += jnp.where(last_x, highs[0], zero) + jnp.where(first_x, lows[0], zero)
    values = [
        jnp.where(last_x, zero, highs[0]), jnp.where(first_x, zero, lows[0]), highs[1], lows[1], highs[2], lows[2],
        center, center + jnp.where(first_y, lows[1], zero), center + jnp.where(last_y, highs[1], zero),
        jnp.where(last_y, zero, highs[1]), jnp.where(first_y, zero, lows[1]),
    ]
    for i, value in enumerate(values):
        coefs[i] = value


def prepared(fields):
    rows, padded_rows = round_up(fields, 8), round_up(fields, 16)
    return (
        jax.ShapeDtypeStruct((11, rows, LANES), jnp.float32),
        jax.ShapeDtypeStruct((rows, 3 * padded_rows), jnp.bfloat16),
    ), [pltpu.VMEM((rows, round_up(3 * padded_rows, LANES)), jnp.float32)]


def fine_kernel(fine, coarse, matrix, coefs, react, reflux, out, reflux_out, state, middle, ready, sems, reflux_sem):
    reflux_copy = pltpu.make_async_copy(reflux, reflux_out, reflux_sem.at[0])
    reflux_copy.start()
    at_bottom, at_top = pencil_ends()
    slots = out.shape[2] * LANES // state.shape[2]
    shifts = matrix[:, -2 * LANES :]
    fields = out.shape[0]
    layers = out.shape[1]
    step = out.shape[2]

    def copy_out(layer, group):
        some = pl.ds(8 * group, min(8, fields - 8 * group))
        return pltpu.make_async_copy(ready.at[layer, some], out.at[some, layer], sems.at[layer, group])

    for slot in range(slots):
        fill_layers(coarse.at[slot], matrix, state, at_bottom, at_top)

        def to_middle(layer, group, across):
            store_group(middle, layer, group, across)

        run_layers(state, 1, layers + 2, coefs, react, fine, to_middle, (layers + 2) // 2, None, True)

        @pl.when(at_bottom)
        def _():
            middle[0] = middle[1]

        @pl.when(at_top)
        def _():
            middle[layers + 1] = middle[layers]

        def to_output(layer, group, across):
            low, high = 8 * group, min(8 * group + 8, fields)
            halves = []
            for t, value in enumerate(across):
                span = slice(LANES * t, LANES * (t + 1))
                halves.append((value + state[layer + 2, low : low + 8, span]) * 0.5)
            lines = ready.at[layer].reshape(fields * step, LANES)
            for t, value in enumerate(to_planes(halves, fine)):
                lines[pl.ds(low * step + t * slots + slot, high - low, stride=step), :] = value[: high - low]
            if slot == slots - 1:
                copy_out(layer, group).start()

        run_layers(middle, 1, layers, coefs, react, fine, to_output, layers, shifts, True)

    for layer in range(layers):
        for group in range(sems.shape[1]):
            copy_out(layer, group).wait()
    reflux_copy.wait()


def side_sums(fine, coarse, matrix, coefs, react, sides, velocity, flux, out, state, sums):
    at_bottom, at_top = pencil_ends()
    fields = out.shape[0]
    rows, width = state.shape[1:]
    layers = state.shape[0] - 4
    fill_layers(coarse, matrix, state, at_bottom, at_top)

    def to_sums(layer, group, across):
        band = slice(8 * group, 8 * group + 8)
        for t, value in enumerate(across):
            span = slice(LANES * t, LANES * (t + 1))
            sums[layer, band, span] = value + state[layer + 2, band, span]

    run_layers(state, 2, layers, coefs, react, fine, to_sums, 2)
    pads = jnp.zeros((round_up(rows, 16) - rows, width), jnp.float32)
    halves = []
    for pair in range(layers // 2):
        high, low = split_halves(jnp.concatenate([sums[2 * pair] + sums[2 * pair + 1], pads], 0))
        halves += [high, low]
    picked = jnp.dot(jnp.concatenate(halves, 0), sides[...], preferred_element_type=jnp.float32)
    step = rows + pads.shape[0]
    each = [
        picked[2 * step * i : 2 * step * i + rows] + picked[2 * step * i + step : 2 * step * i + step + rows]
        for i in range(layers // 2)
    ]
    span = sides.shape[1]
    per_tile = span // (fine * 2)
    lane = lax.broadcasted_iota(jnp.int32, (rows, span), 1)
    for tile in range(len(each) // per_tile):
        value = each[tile * per_tile]
        for i in range(1, per_tile):
            value = jnp.where(lane >= i * fine * 2, each[tile * per_tile + i], value)
        along_x = lax.rem(lane, fine * 2) < fine
        value = value * jnp.where(along_x, velocity[0] * 0.125, velocity[1] * 0.125)
        out[:, tile, :] = value[:fields] - flux[:, tile, :]


def route_kernel(
    fine, owner_hbm, velocity_hbm, own_hbm, diffusivity_hbm, stoich_hbm, flux_hbm, matrix_hbm, sides_hbm,
    held, reflux, coefs, react, matrix, table, state, sums, mine,
    owner, velocity, own, diffusivity, stoich, flux, sides, w_sems,
    outgoing, edges, arrived, chosen, landed, a_send, a_recv, h_send, h_recv, b_send, b_recv,
):
    me, pencil = lax.axis_index("gx"), lax.axis_index("gy")
    groups, pencils = lax.axis_size("gx"), lax.axis_size("gy")
    fields = own.shape[0]
    rows, sent = outgoing.shape[1], round_up(fields, 4)
    half = groups // 2
    pairs = (
        (own_hbm, own), (owner_hbm, owner), (velocity_hbm, velocity), (diffusivity_hbm, diffusivity),
        (stoich_hbm, stoich), (flux_hbm, flux), (matrix_hbm, matrix), (sides_hbm, sides),
    )
    fetches = [pltpu.make_async_copy(source, target, w_sems.at[i]) for i, (source, target) in enumerate(pairs)]
    for copy in fetches:
        copy.start()
    own_in, owner_in, small_in, weights = fetches[0], fetches[1], fetches[2:5], fetches[5:]
    slots = chosen.shape[1]
    has_low, has_high = pencil > 0, pencil < pencils - 1
    around = [lax.rem(me + k, groups) for k in range(groups)]

    barrier = pltpu.get_barrier_semaphore()

    def greet(group, to):
        pl.semaphore_signal(barrier, inc=1, device_id=(group, to), device_id_type=pl.DeviceIdType.MESH)

    for group in around[1:]:
        greet(group, pencil)

    @pl.when(has_low)
    def _():
        greet(me, pencil - 1)

    @pl.when(has_high)
    def _():
        greet(me, pencil + 1)

    own_in.wait()
    for piece in range(groups):
        outgoing[piece, :fields] = own[:, LANES * piece : LANES * (piece + 1)]
        outgoing[piece, fields:] = jnp.zeros((rows - fields, LANES), jnp.bfloat16)
    arrived[me] = outgoing[me]
    arrived[groups] = jnp.zeros(arrived.shape[1:], jnp.bfloat16)

    near = groups - 1
    pl.semaphore_wait(barrier, near + (has_low.astype(jnp.int32) + has_high.astype(jnp.int32)))

    def send(src, dst, out_sem, in_sem, group, to):
        return pltpu.make_async_remote_copy(
            src_ref=src, dst_ref=dst, send_sem=out_sem, recv_sem=in_sem,
            device_id=(group, to), device_id_type=pl.DeviceIdType.MESH,
        )

    first = [
        send(outgoing.at[group, :sent], arrived.at[me, :sent], a_send.at[k], a_recv.at[me], group, pencil)
        for k, group in enumerate(around)
    ]
    to_high = send(outgoing.at[half:, :sent], edges.at[:half, :sent], h_send.at[0], h_recv.at[0], me, pencil + 1)
    to_low = send(outgoing.at[:half, :sent], edges.at[half:, :sent], h_send.at[1], h_recv.at[1], me, pencil - 1)
    for k in sorted(range(1, groups), key=lambda k: min(k, groups - k)):
        first[k].start()
    pl.when(has_high)(to_high.start)
    pl.when(has_low)(to_low.start)
    owner_in.wait()
    sources = []
    for group in around:
        for o in range(slots):
            slot = group * slots + o
            source = jnp.int32(groups)
            for q in range(groups):
                source = jnp.where(owner[q] == slot, q, source)
            sources.append(source)

    for copy in small_in:
        copy.wait()
    prepare(velocity, diffusivity, stoich, coefs, react, table, fine)
    for group in around[1:]:
        send(outgoing.at[group, :sent], arrived.at[group, :sent], a_send.at[0], a_recv.at[group], group, pencil).wait_recv()

    for k, group in enumerate(around):
        for o in range(slots):
            chosen[group, o, :sent] = arrived[sources[k * slots + o], :sent]
    landed[half + me, :, :sent] = chosen[me, :, :sent]

    second = [
        send(chosen.at[group, :, :sent], landed.at[half + me, :, :sent], b_send.at[0, k], b_recv.at[half + me], group, pencil)
        for k, group in enumerate(around)
    ]
    for copy in second[1:]:
        copy.start()

    relays = []
    for k, group in enumerate(around):
        piece = landed.at[half + group, :, :sent]
        goes_low = jnp.logical_and(has_low, group < half)
        goes_high = jnp.logical_and(has_high, group >= half)
        over, under = half + groups + group, lax.rem(group + half, groups)
        relays.append((goes_low, send(piece, landed.at[over, :, :sent], b_send.at[1, k], b_recv.at[over], me, pencil - 1)))
        relays.append((goes_high, send(piece, landed.at[under, :, :sent], b_send.at[1, k], b_recv.at[under], me, pencil + 1)))

    def arrival(piece):
        return send(chosen.at[0, :, :sent], landed.at[piece, :, :sent], b_send.at[0, 0], b_recv.at[piece], me, pencil)

    def place(index, piece, value):
        layer, part = divmod(piece, half // 2)
        span = slice(LANES * part, LANES * (part + 1))
        if index == slots:
            mine[layer, : value.shape[0], span] = value
        else:
            held[index, layer, : value.shape[0], span] = value

    blank = jnp.zeros((rows, LANES), jnp.bfloat16)
    for layer in range(mine.shape[0]):
        for index in range(slots):
            held[index, layer, sent:, :] = jnp.zeros((rows - sent, held.shape[3]), jnp.bfloat16)
        mine[layer, sent:, :] = jnp.zeros((rows - sent, held.shape[3]), jnp.bfloat16)
    for piece in range(groups):
        place(slots, half + piece, outgoing[piece])

    def edge_pieces(present, incoming, pieces, start):
        @pl.when(present)
        def _():
            incoming.wait_recv()
            for piece in pieces:
                place(slots, piece, edges[start + piece - pieces[0], :sent])

        @pl.when(jnp.logical_not(present))
        def _():
            for piece in pieces:
                for index in range(slots + 1):
                    place(index, piece, blank)

    low_pieces = list(range(half))
    high_pieces = list(range(half + groups, 2 * half + groups))
    edge_pieces(has_low, to_high, low_pieces, 0)
    edge_pieces(has_high, to_low, high_pieces, half)
    for copy in weights:
        copy.wait()
    side_sums(fine, mine, matrix, coefs, react, sides, velocity, flux, reflux, state, sums)

    for k, group in enumerate(around):
        if k:
            arrival(half + group).wait_recv()
        for present, copy in relays[2 * k : 2 * k + 2]:
            pl.when(present)(copy.start)
    for piece in range(groups):
        for o in range(slots):
            place(o, half + piece, landed[half + piece, o, :sent])
    for present, pieces in ((has_low, low_pieces), (has_high, high_pieces)):

        @pl.when(present)
        def _(pieces=pieces):
            for piece in pieces:
                arrival(piece).wait_recv()
                for o in range(slots):
                    place(o, piece, landed[piece, o, :sent])

    for copy in first[1:] + second[1:]:
        copy.wait_send()
    pl.when(has_high)(to_high.wait_send)
    pl.when(has_low)(to_low.wait_send)

    for present, copy in relays:
        pl.when(present)(copy.wait_send)


def route_by_kernel(fine, work, params, coarse_send, flux, patch_owner, velocity, diffusivity, stoich, matrix, sides, own_slots):
    groups = lax.axis_size("gx")
    fields, cells = coarse_send.shape[1:]
    plane = fine * fine // 4
    padded_rows = round_up(fields, 16)
    held_layers = 2 * cells // plane
    piece = (padded_rows, LANES)
    vmem = pl.BlockSpec(memory_space=pltpu.VMEM)
    anywhere = pl.BlockSpec(memory_space=pltpu.HBM)
    dma = pltpu.SemaphoreType.DMA
    bf16 = jnp.bfloat16
    tables, table = prepared(fields)
    return pl.pallas_call(
        functools.partial(route_kernel, fine),
        out_shape=(
            pltpu.VMEM((own_slots, held_layers, padded_rows, plane), bf16),
            pltpu.VMEM(flux.shape, jnp.float32),
        )
        + tuple(pltpu.VMEM(t.shape, t.dtype) for t in tables)
        + (pltpu.VMEM(matrix.shape, bf16),),
        in_specs=[anywhere] * 8,
        out_specs=(vmem,) * 5,
        scratch_shapes=table
        + work
        + [
            pltpu.VMEM((2 * cells // plane, round_up(fields, 8), fine * fine), jnp.float32),
            pltpu.VMEM((held_layers, padded_rows, plane), bf16),
            pltpu.SMEM(patch_owner.shape, jnp.int32),
            pltpu.SMEM(velocity.shape, jnp.float32),
            pltpu.VMEM((fields, cells), bf16),
            pltpu.VMEM(diffusivity.shape, jnp.float32),
            pltpu.VMEM(stoich.shape, jnp.float32),
            pltpu.VMEM(flux.shape, jnp.float32),
            pltpu.VMEM(sides.shape, bf16),
            dma((8,)),
            pltpu.VMEM((groups,) + piece, bf16),
            pltpu.VMEM((groups,) + piece, bf16),
            pltpu.VMEM((groups + 1,) + piece, bf16),
            pltpu.VMEM((groups, own_slots) + piece, bf16),
            pltpu.VMEM((2 * groups, own_slots) + piece, bf16),
            dma((groups,)),
            dma((groups,)),
            dma((2,)),
            dma((2,)),
            dma((2, groups)),
            dma((2 * groups,)),
        ],
        compiler_params=params(collective_id=0, has_side_effects=True),
        name="route",
    )(*(
        pltpu.with_memory_space_constraint(x, pltpu.HBM)
        for x in (patch_owner, velocity, coarse_send[0], diffusivity, stoich, flux, matrix, sides)
    ))


def side_kernel(fine, velocity, coarse, matrix, diffusivity, stoich, sides, flux, out, coefs, react, table, state, sums):
    prepare(velocity, diffusivity, stoich, coefs, react, table, fine)
    side_sums(fine, coarse, matrix, coefs, react, sides, velocity, flux, out, state, sums)


def route_by_gather(coarse_send, patch_owner, own_slots, padded_rows, plane):
    pencils = lax.axis_size("gy")
    fields, cells = coarse_send.shape[1:]
    my_slots = lax.axis_index("gx") * own_slots + jnp.arange(own_slots, dtype=jnp.int32)
    chooser = (my_slots[:, None] == patch_owner[None, :]).astype(jnp.bfloat16)
    owned = jnp.einsum(
        "oq,qfc->ofc", chooser, lax.all_gather(coarse_send, "gx", axis=0, tiled=True),
        preferred_element_type=jnp.float32,
    ).astype(jnp.bfloat16)
    both = jnp.concatenate([owned, coarse_send], 0)
    forward = [(i, i + 1) for i in range(pencils - 1)]
    backward = [(i + 1, i) for i in range(pencils - 1)]
    below = lax.ppermute(both[:, :, -2 * plane:], "gy", forward)
    above = lax.ppermute(both[:, :, : 2 * plane], "gy", backward)
    held = jnp.concatenate([below, both, above], 2)
    held = jnp.pad(held, ((0, 0), (0, padded_rows - fields), (0, 0)))
    return held.reshape(-1, padded_rows, cells // plane + 4, plane).transpose(0, 2, 1, 3)


def shards(coarse_send, coarse_flux, patch_owner, velocity, diffusivity, stoich):
    send_slots, fields, layer_cells = coarse_send.shape
    pencils = lax.axis_size("gy")
    edge = round((layer_cells * pencils) ** (1.0 / 3.0))
    fine, plane = 2 * edge, edge * edge
    layers = layer_cells // plane
    own_slots = 2 * send_slots
    rows, padded_rows = round_up(fields, 8), round_up(fields, 16)
    width = fine * fine
    deep = 2 * layers

    matrix = jnp.asarray(refine_matrix(edge), jnp.bfloat16)
    sides = jnp.asarray(side_matrix(edge), jnp.bfloat16)
    diffusivity = diffusivity.reshape(1, fields)
    fluxes = coarse_flux.reshape(send_slots, fields, -1, LANES)
    vmem = pl.BlockSpec(memory_space=pltpu.VMEM)
    smem = pl.BlockSpec(memory_space=pltpu.SMEM)
    work = [pltpu.VMEM((deep + 4, rows, width), jnp.float32)]
    params = functools.partial(pltpu.CompilerParams, vmem_limit_bytes=48 * 1024 * 1024)

    fits = send_slots == 1 and lax.axis_size("gx") * LANES == layer_cells and layers == 4 and plane == 2 * LANES
    if fits:
        held, reflux, coefs, react, matrix = route_by_kernel(
            fine, work, params, coarse_send, fluxes[0], patch_owner, velocity, diffusivity, stoich, matrix, sides, own_slots
        )
        reflux = reflux[None]
    else:
        held = route_by_gather(coarse_send, patch_owner, own_slots, padded_rows, plane)
        tables, table = prepared(fields)
        reflux = []
        for i in range(send_slots):
            one, coefs, react = pl.pallas_call(
                functools.partial(side_kernel, fine),
                out_shape=(jax.ShapeDtypeStruct(fluxes.shape[1:], jnp.float32),) + tables,
                in_specs=[smem] + [vmem] * 6,
                out_specs=(vmem,) * 3,
                scratch_shapes=table + work + [pltpu.VMEM((deep, rows, width), jnp.float32)],
                compiler_params=params(),
                name="sides",
            )(velocity, held[own_slots + i], matrix, diffusivity, stoich, sides, fluxes[i])
            reflux.append(one)
        reflux = jnp.stack(reflux)
        held = held[:own_slots]
    anywhere = pl.BlockSpec(memory_space=pl.ANY)
    state, reflux = pl.pallas_call(
        functools.partial(fine_kernel, fine),
        out_shape=(
            jax.ShapeDtypeStruct((fields, deep, own_slots * width // LANES, LANES), jnp.float32),
            jax.ShapeDtypeStruct(reflux.shape, jnp.float32),
        ),
        in_specs=[vmem] * 5,
        out_specs=(anywhere, anywhere),
        scratch_shapes=work
        + [
            pltpu.VMEM((deep + 2, rows, width), jnp.float32),
            pltpu.VMEM((deep, fields, own_slots * width // LANES, LANES), jnp.float32),
            pltpu.SemaphoreType.DMA((deep, rows // 8)),
            pltpu.SemaphoreType.DMA((1,)),
        ],
        compiler_params=params(),
        name="fine",
    )(held, matrix, coefs, react, reflux)
    state = state.reshape(fields, deep * width // LANES, own_slots, LANES).transpose(2, 0, 1, 3)
    return state.reshape(own_slots, fields, deep * width), reflux.reshape(send_slots, fields, -1)


def solution(mesh):
    placed = (P("gx", None, "gy"), P("gx", None, "gy"), P(), P(), P(), P())
    return jax.shard_map(
        shards,
        mesh=mesh,
        in_specs=placed,
        out_specs=(P("gx", None, "gy"), P("gx", None, "gy")),
        check_vma=False,
    )
```
